32 devices in a mesh: dp: 8 (over y, x, core), tensor: 4 (over z).
Axes of the slice: x: 2, y: 2, z: 4, core: 2. Of those that a mesh axis runs over, the one named last changes fastest.
Arguments:
- acts: bfloat16 [1024, 4096], P('dp'), may hold values from -6 to 6
- grad_out: bfloat16 [1024, 14336], P('dp', 'tensor'), may hold values from -0.1875 to 0.1875
- selected: int32 [4, 4], P('tensor'), may hold values from 0 to 27, as said below
- owner: int32 [4, 192, 1], P('tensor'), may hold values from 0 to 7; in each aligned block of 192 rows (0 to 191, 192 to 383, ..., all dimensions but the last counted through in order) at most 36 rows name the same one
- sel_weight: float32 [4096, 2048], P('dp', 'tensor'), may hold values from -3 to 3
- sel_moment: float32 [4096, 2048], P('dp', 'tensor'), may hold values from -3 to 3
- sel_second: float32 [4096, 2048], P('dp', 'tensor'), may hold values from 0.01 to 1
- off_weight: float32 [8, 4, 36, 512, 128], P('dp', 'tensor'), may hold values from -3 to 3
- off_moment: float32 [8, 4, 36, 512, 128], P('dp', 'tensor'), may hold values from -3 to 3
- off_second: float32 [8, 4, 36, 512, 128], P('dp', 'tensor'), may hold values from 0.01 to 1
Outputs:
- column_norm: float32 [14336], P('tensor')
- sel_weight_new: float32 [4096, 2048], P('dp', 'tensor')
- sel_moment_new: float32 [4096, 2048], P('dp', 'tensor')
- sel_second_new: float32 [4096, 2048], P('dp', 'tensor')
- off_weight_new: float32 [8, 4, 36, 512, 128], P('dp', 'tensor')
- off_moment_new: float32 [8, 4, 36, 512, 128], P('dp', 'tensor')
- off_second_new: float32 [8, 4, 36, 512, 128], P('dp', 'tensor')
The draws below stay inside these ranges and needn't reach their ends.
Inputs may be any that keep to these rules, and one draw needn't show every extreme that they name: `selected`: each row names 4 tile. For each index of tensor, no owner receives more than 36 pieces, and some owner receives exactly 36.
All inputs are finite; a program needn't handle non-finite values.
Results may differ from the reference program's by a relative error of at most 0.0017.
Values may be sent and summed in bfloat16 or wider, within the bound.
A program may use at most 192 MiB of HBM per device.

```python
import math
import jax
import jax.numpy as jnp
import numpy as np
from jax import lax

ROWS = 4096
FFW = 14336
TILE = 128
TOK_DEV = 128
TOKENS = 1024
TILES_DEV = 28
SEL_TILES = 4
REST_TILES = 24
BLOCK_ROWS = 512
PIECES = 192
CAP = 36
N_DP = 8
N_TENSOR = 4


def draw_selected(key, part):
    row_keys = jax.random.split(jax.random.fold_in(key, 17), N_TENSOR)
    shuffled = jax.vmap(lambda row_key: jax.random.permutation(row_key, TILES_DEV))(row_keys)
    return jnp.sort(shuffled[:, :SEL_TILES], axis=1).astype(jnp.int32)


def shard_levels(key, extent, cuts, low, high):
    def one(axis_at, parts):
        heights = jax.random.uniform(jax.random.fold_in(jax.random.fold_in(key, 6), axis_at), (parts,), jnp.float32, low / len(cuts), high / len(cuts))
        return jnp.repeat(jnp.exp(heights), extent[axis_at] // parts).reshape((-1,) + (1,) * (len(extent) - axis_at - 1))

    factor_of = one(*cuts[0])
    for cut in cuts[1:]:
        factor_of = factor_of * one(*cut)
    return factor_of


def deal_out(own_key, own, number, rows, amount, top, bound, slope):
    order = jax.random.permutation(own_key, amount)
    crowded, usual = shares(amount, rows * top, bound, slope, True), shares(amount, rows * top, bound, slope, False)
    places = jnp.arange(amount)

    def named(lengths, rotation):
        used = int((lengths > 0).sum())
        fixed = max(1, used // 4)
        shifted = fixed + (places - fixed + rotation * (used - fixed)) % max(1, amount - fixed)
        return jnp.zeros((amount,), jnp.int32).at[order[jnp.where(places < fixed, places, shifted)]].set(jnp.asarray(lengths, jnp.int32))

    lengths = jnp.where(number % 4 == 0, named(crowded, number // 4), named(usual, number - number // 4 - 1))
    mixed = jax.random.permutation(jax.random.fold_in(own, 3), amount)
    giver, receiver = mixed[0:amount // 2 * 2:2], mixed[1:amount // 2 * 2:2]
    slack = jnp.minimum(lengths[giver] - 1, bound - lengths[receiver]) // 2
    slack = jnp.where((giver == order[0]) | (receiver == order[0]) | (lengths[receiver] == 0), 0, jnp.maximum(slack, 0))
    shifted = jax.random.randint(jax.random.fold_in(own, 4), (amount // 2,), 0, 1 << 20) % (slack + 1)
    lengths = lengths.at[giver].add(-shifted).at[receiver].add(shifted)
    members = jnp.searchsorted(jnp.cumsum(lengths), jnp.arange(rows * top), side="right").astype(jnp.int32)
    table = members.reshape(top, rows).T
    table = table[jax.random.permutation(jax.random.fold_in(own, 1), rows)]
    rotation = jax.random.randint(jax.random.fold_in(own, 2), (rows, 1), 0, top)
    return jnp.take_along_axis(table, (jnp.arange(top)[None, :] + rotation) % top, axis=1)


def shares(amount, total, bound, skew, full):
    loads = [(1 << 20) // math.isqrt(grade ** skew) + 1 for grade in range(1, amount + 1)]
    largest = bound if full else min(bound, max(-(-total // amount), total * loads[0] // sum(loads)))
    least = 1 if total - largest >= amount - 1 else 0
    given, rest = [largest] + [least] * (amount - 1), total - largest - least * (amount - 1)
    while rest > 0:
        movable = [i for i in range(1, amount) if given[i] < largest] or [i for i in range(1, amount) if given[i] < bound]
        whole, left = sum([loads[i] for i in movable]), rest
        for i in movable:
            extra = min(bound - given[i], max(1, left * loads[i] // whole), rest)
            given[i] = given[i] + extra
            rest = rest - extra
    return np.array(given)


def centred(rng, dims, deviation, bound, cuts=(), kind=jnp.bfloat16):
    entries = deviation * jax.random.normal(rng, dims, jnp.float32)
    if cuts:
        entries = entries * shard_levels(rng, dims, cuts, -0.22, 0.18)
    return jnp.clip(entries, -bound, bound).astype(kind)


def setup_inputs(seed: int = 0) -> dict:
    keys = jax.random.split(jax.random.key(seed), 11)
    acts = centred(keys[0], (TOKENS, ROWS), 1.0, 6.0, ((0, 8),))
    grad_out = centred(keys[1], (TOKENS, FFW), TOKENS ** -0.5, 0.1875, ((0, 8), (1, 4)))
    selected = draw_selected(jax.random.fold_in(keys[10], 71), 0)
    owner_keys = jax.random.split(jax.random.fold_in(keys[3], 1), N_TENSOR * PIECES // PIECES)
    owner_turns = jax.random.permutation(jax.random.fold_in(keys[3], 3), N_TENSOR * PIECES // PIECES)
    owner = jax.vmap(lambda own, number: deal_out(jax.random.fold_in(keys[3], 2), own, number, PIECES, N_DP, 1, CAP, 2))(owner_keys, owner_turns).reshape((N_TENSOR, PIECES, 1))
    sel_weight = centred(keys[4], (ROWS, N_TENSOR * SEL_TILES * TILE), 0.5, 3.0, ((0, 8), (1, 4)), jnp.float32)
    sel_moment = centred(keys[5], (ROWS, N_TENSOR * SEL_TILES * TILE), 0.5, 3.0, ((0, 8), (1, 4)), jnp.float32)
    sel_second = jnp.clip(jnp.exp(math.log(1.0) - 4.6051702 * jax.random.uniform(keys[6], (ROWS, N_TENSOR * SEL_TILES * TILE), jnp.float32) ** shard_levels(keys[6], (ROWS, N_TENSOR * SEL_TILES * TILE), ((0, 8), (1, 4)), -0.2, 0.2)), 0.01, 1.0)
    off_weight = centred(keys[7], (N_DP, N_TENSOR, CAP, BLOCK_ROWS, TILE), 0.5, 3.0, ((0, 8), (1, 4)), jnp.float32)
    off_moment = centred(keys[8], (N_DP, N_TENSOR, CAP, BLOCK_ROWS, TILE), 0.5, 3.0, ((0, 8), (1, 4)), jnp.float32)
    off_second = jnp.clip(jnp.exp(math.log(1.0) - 4.6051702 * jax.random.uniform(keys[9], (N_DP, N_TENSOR, CAP, BLOCK_ROWS, TILE), jnp.float32) ** shard_levels(keys[9], (N_DP, N_TENSOR, CAP, BLOCK_ROWS, TILE), ((0, 8), (1, 4)), -0.2, 0.2)), 0.01, 1.0)
    return dict(acts=acts, grad_out=grad_out, selected=selected, owner=owner, sel_weight=sel_weight, sel_moment=sel_moment, sel_second=sel_second, off_weight=off_weight, off_moment=off_moment, off_second=off_second)


beta_one = 0.9
beta_two = 0.95
adam_eps = 1e-08
learn_rate = 0.01
decay_rate = 0.1
step_count = 10.0

def adam_update(weight, moment, second, grad):
    moment_new = beta_one * moment + (1.0 - beta_one) * grad
    second_new = beta_two * second + (1.0 - beta_two) * grad * grad
    first_fix = 1.0 - beta_one ** step_count
    second_fix = 1.0 - beta_two ** step_count
    update = moment_new / first_fix / (jnp.sqrt(second_new / second_fix) + adam_eps)
    return (weight - learn_rate * (update + decay_rate * weight), moment_new, second_new)

def rest_tiles(selected_row):
    tiles = jnp.arange(TILES_DEV, dtype=jnp.int32)
    chosen = jnp.any(tiles[:, None] == selected_row[None, :], axis=1).astype(jnp.int32)
    order = jnp.argsort(chosen * TILES_DEV + tiles).astype(jnp.int32)
    return order[:REST_TILES]

def slot_numbers(owner_row):
    places = jnp.arange(owner_row.shape[0], dtype=jnp.int32)
    earlier = (owner_row[:, None] == owner_row[None, :]) & (places[:, None] > places[None, :])
    return lax.optimization_barrier(jnp.sum(earlier.astype(jnp.int32), axis=1)).astype(jnp.int32)

def place_pieces(piece_row, owner_row):
    target = (owner_row * CAP + slot_numbers(owner_row)).astype(jnp.int32)
    empty = jnp.zeros((N_DP * CAP, BLOCK_ROWS, TILE), jnp.bfloat16)
    return empty.at[target].set(piece_row).reshape(N_DP, CAP, BLOCK_ROWS, TILE)

def reference(acts, grad_out, selected, owner, sel_weight, sel_moment, sel_second, off_weight, off_moment, off_second):
    rest_lists = jax.vmap(rest_tiles)(selected)
    acts_shards = acts.reshape(N_DP, TOK_DEV, ROWS)
    grad_shards = grad_out.reshape(N_DP, TOK_DEV, FFW)
    sel_index = selected.astype(jnp.int32)[None, :, :, None]
    rest_index = rest_lists.astype(jnp.int32)[None, :, :, None]

    def add_shard(carry, shard):
        squares, sel_sum, rest_sum = carry
        partial_value = jnp.dot(shard[0].T, shard[1], preferred_element_type=jnp.float32)
        squares = squares + lax.optimization_barrier(jnp.sum(partial_value * partial_value, axis=0))
        tiled = partial_value.reshape(ROWS, N_TENSOR, TILES_DEV, TILE)
        sel_part = jnp.take_along_axis(tiled, sel_index, axis=2).reshape(ROWS, N_TENSOR * SEL_TILES * TILE)
        rest_part = jnp.take_along_axis(tiled, rest_index, axis=2).astype(jnp.bfloat16)
        rest_part = lax.optimization_barrier(rest_part).astype(jnp.float32)
        return ((squares, sel_sum + sel_part, rest_sum + rest_part), None)
    start = (jnp.zeros((FFW,), jnp.float32), jnp.zeros((ROWS, N_TENSOR * SEL_TILES * TILE), jnp.float32), jnp.zeros((ROWS, N_TENSOR, REST_TILES, TILE), jnp.float32))
    (squares, sel_sum, rest_sum), unused = lax.scan(add_shard, start, (acts_shards, grad_shards))
    column_norm = jnp.sqrt(squares)
    new_sel = adam_update(sel_weight, sel_moment, sel_second, sel_sum)
    pieces = rest_sum.astype(jnp.bfloat16).reshape(N_DP, BLOCK_ROWS, N_TENSOR, REST_TILES, TILE)
    pieces = jnp.transpose(pieces, (2, 3, 0, 1, 4)).reshape(N_TENSOR, PIECES, BLOCK_ROWS, TILE)
    slots = jax.vmap(place_pieces)(pieces, owner[:, :, 0].astype(jnp.int32))
    offload = jnp.transpose(slots, (1, 0, 2, 3, 4)).astype(jnp.float32)
    new_off = adam_update(off_weight, off_moment, off_second, offload)
    return (column_norm, new_sel[0], new_sel[1], new_sel[2], new_off[0], new_off[1], new_off[2])
```

```python
import functools

import jax
import jax.numpy as jnp
from jax import lax
from jax.experimental import pallas as pl
from jax.experimental.pallas import tpu as pltpu
from jax.sharding import PartitionSpec as P

TILE = 128
DEPTH = 4
ROWS_ONCE = 128
MIB = 1024 * 1024

beta_one = 0.9
beta_two = 0.95
adam_eps = 1e-08
learn_rate = 0.01
decay_rate = 0.1
step_count = 10.0

MESH = pl.DeviceIdType.MESH


def adam_update(weight, moment, second, grad):
    first_fix = 1.0 - beta_one**step_count
    second_fix = 1.0 - beta_two**step_count
    moment_new = beta_one * moment + (1.0 - beta_one) * grad
    second_new = beta_two * second + (1.0 - beta_two) * (grad * grad)
    scale = jnp.sqrt(second_new * (1.0 / second_fix)) + adam_eps
    update = moment_new * (learn_rate / first_fix) / scale
    return weight * (1.0 - learn_rate * decay_rate) - update, moment_new, second_new


def flip_bits(index, mask):
    result, bit = index, 1
    while bit <= mask:
        if mask & bit:
            result = result + bit * (1 - 2 * ((index // bit) % 2))
        bit *= 2
    return result


def rounded(value):
    return value.astype(jnp.bfloat16).astype(jnp.float32)


def in_hbm(array):
    return pltpu.with_memory_space_constraint(array, pltpu.HBM)


def unroll_of(count):
    return next(k for k in (3, 2, 1) if count % k == 0)


def table_kernel(
    n, capacity, sel_tile, owner, table, next_piece, next_free, rest_tile
):
    me = lax.axis_index("dp")
    sel_count = sel_tile.shape[0]
    piece_count, tiles_here = owner.shape[0], next_free.shape[0] - 1

    def piece_step(i, following):
        p = piece_count - 1 - i
        following = jnp.where(owner[p] == me, p, following)
        next_piece[p] = following
        return following

    next_piece[piece_count] = piece_count
    next_piece[piece_count + 1] = piece_count
    lax.fori_loop(0, piece_count, piece_step, jnp.int32(piece_count))

    def free_step(i, following):
        t = tiles_here - 1 - i
        taken = jnp.int32(0)
        for k in range(sel_count):
            taken = taken + (sel_tile[k] == t).astype(jnp.int32)
        following = jnp.where(taken == 0, t, following)
        next_free[t] = following
        return following

    next_free[tiles_here] = 0
    lax.fori_loop(0, tiles_here, free_step, jnp.int32(0))

    def rest_step(k, at):
        tile = next_free[at]
        rest_tile[k] = tile
        return tile + 1

    lax.fori_loop(0, tiles_here - sel_count, rest_step, jnp.int32(0))

    def slot_step(s, at):
        p = next_piece[at]
        found = p < piece_count
        piece = jnp.where(found, p, 0)
        table[s] = rest_tile[lax.div(piece, n)]
        table[capacity + s] = lax.rem(piece, n)
        table[2 * capacity + s] = found.astype(jnp.int32)
        return p + 1 - (p // piece_count)

    lax.fori_loop(0, capacity, slot_step, jnp.int32(0))
    for k in range(sel_count):
        table[3 * capacity + k] = sel_tile[k]


def gather_kernel(n, paired, late, table_source, acts, grad, *refs):
    states, refs = refs[:5], refs[5:]
    late_a, late_g = refs[: len(late)], refs[len(late) : 2 * len(late)]
    refs = refs[2 * len(late) :]
    kept = refs[:5]
    total, sel_sum, norm = refs[5:8]
    early = [mask for mask in range(n) if mask not in late]
    refs = refs[8:]
    table, raw, squares = refs[:3]
    send_sem, recv_sem, send_q, recv_q, load_sem, grad_sem = refs[3:9]
    held_a = dict(zip(early, refs[9 : 9 + len(early)])) | dict(zip(late, late_a))
    held_g = dict(zip(early, refs[9 + len(early) :])) | dict(zip(late, late_g))

    layer = lax.axis_index("tensor")
    me = lax.axis_index("dp")
    capacity = total.shape[0]
    sel_count = sel_sum.shape[1] // TILE
    row_block = total.shape[1]
    tiles_here = grad.shape[1] // TILE
    kinds = ("a0", "a1", "z0", "z1", "g0", "g1")
    if paired:
        side, part = layer % 2, n // 4
        cut = tiles_here // 2
        parts = {
            "a0": (held_a, (pl.ds(side * 2 * part, part),)),
            "a1": (held_a, (pl.ds(side * 2 * part + part, part),)),
            "z0": (held_a, (pl.ds((1 - side) * 2 * part, part),)),
            "z1": (held_a, (pl.ds((1 - side) * 2 * part + part, part),)),
            "g0": (held_g, (pl.ds(0, cut),)),
            "g1": (held_g, (pl.ds(cut, tiles_here - cut),)),
        }
    else:
        parts = {
            "a0": (held_a, (slice(None),)),
            "g0": (held_g, (slice(None),)),
        }

    own_acts = pltpu.make_async_copy(acts, raw, load_sem.at[0])
    own_table = pltpu.make_async_copy(table_source, table, load_sem.at[1])
    own_grads = [
        pltpu.make_async_copy(
            grad.at[:, pl.ds(tile * TILE, TILE)], held_g[0].at[tile], grad_sem.at[tile]
        )
        for tile in range(tiles_here)
    ]
    own_acts.start()
    own_table.start()
    for copy in own_grads:
        copy.start()
    loads = []
    for number, (source, target) in enumerate(zip(states, kept)):
        load = pltpu.make_async_copy(source, target, load_sem.at[2 + number])
        loads.append(load)

    barrier = pltpu.get_barrier_semaphore()
    for mask in range(1, n):
        pl.semaphore_signal(
            barrier, inc=1, device_id={"dp": flip_bits(me, mask)}, device_id_type=MESH
        )
    if paired:
        pl.semaphore_signal(
            barrier, inc=1, device_id={"tensor": flip_bits(layer, 1)}, device_id_type=MESH
        )
    own_acts.wait()
    for block in range(n):
        held_a[0][block] = raw[:, pl.ds(block * row_block, row_block)].T
    for copy in own_grads:
        copy.wait()
    own_table.wait()
    pl.semaphore_wait(barrier, n if paired else n - 1)

    started = []

    def at_part(kind, mask):
        slots, place = parts[kind]
        return slots[mask].at[place]

    def recv_of(kind, mask):
        return recv_sem.at[kinds.index(kind) * (n - 1) + mask - 1]

    def copy_of(kind, mask, peer, number):
        there = mask ^ peer
        slots, place = parts[kind]
        return pltpu.make_async_remote_copy(
            src_ref=slots[mask].at[place],
            dst_ref=slots[there].at[place],
            send_sem=send_sem.at[number],
            recv_sem=recv_of(kind, there),
            device_id={"dp": flip_bits(me, peer)},
            device_id_type=MESH,
        )

    def send(kind, mask, peer):
        copy = copy_of(kind, mask, peer, len(started))
        copy.start()
        started.append(copy)

    def send_across(kind, mask):
        copy = pltpu.make_async_remote_copy(
            src_ref=at_part(kind, mask),
            dst_ref=at_part(kind, mask),
            send_sem=send_sem.at[len(started)],
            recv_sem=recv_of("z" + kind[1], mask),
            device_id={"tensor": flip_bits(layer, 1)},
            device_id_type=MESH,
        )
        copy.start()
        started.append(copy)

    def arrived(kind, mask):
        copy_of(kind, 0, mask, 0).wait_recv()

    def square_columns():
        whole = held_a[0][...].reshape(n * row_block, raw.shape[0])
        gram = jnp.dot(raw[...], whole, preferred_element_type=jnp.float32)
        high = gram.astype(jnp.bfloat16)
        rest = gram - high.astype(jnp.float32)
        middle = rest.astype(jnp.bfloat16)
        low = (rest - middle.astype(jnp.float32)).astype(jnp.bfloat16)

        @pl.loop(0, tiles_here, unroll=unroll_of(tiles_here))
        def _(tile):
            piece = held_g[0][tile]
            product = jnp.dot(low, piece, preferred_element_type=jnp.float32)
            product += jnp.dot(middle, piece, preferred_element_type=jnp.float32)
            product += jnp.dot(high, piece, preferred_element_type=jnp.float32)
            squares[0, pl.ds(tile, 1)] = jnp.sum(
                piece.astype(jnp.float32) * product, axis=0, keepdims=True
            )

    def square_copy(mask):
        return pltpu.make_async_remote_copy(
            src_ref=squares.at[0],
            dst_ref=squares.at[mask],
            send_sem=send_q.at[mask - 1],
            recv_sem=recv_q.at[mask - 1],
            device_id={"dp": flip_bits(me, mask)},
            device_id_type=MESH,
        )

    def add_slots(masks, first, begin, end):
        @pl.loop(begin, end, unroll=unroll_of(end - begin))
        def _(slot):
            block, tile = table[capacity + slot], table[slot]
            value = None if first else total[slot]
            for mask in masks:
                partial = rounded(
                    jnp.dot(
                        held_a[mask][block],
                        held_g[mask][tile],
                        preferred_element_type=jnp.float32,
                    )
                )
                value = partial if value is None else value + partial
            total[slot] = value

    def add_selected(masks, first):
        for i in range(sel_count):
            tile, place = table[3 * capacity + i], pl.ds(i * TILE, TILE)
            value = None if first else sel_sum[:, place]
            for mask in masks:
                partial = jnp.dot(
                    held_a[mask][me],
                    held_g[mask][tile],
                    preferred_element_type=jnp.float32,
                )
                value = partial if value is None else value + partial
            sel_sum[:, place] = value

    def complete(mask, only=kinds):
        for kind in only:
            if kind in parts:
                arrived(kind, mask)

    def relay(kind, mask):
        arrived(kind, mask)
        send(kind, mask, 1)

    if paired:
        core, near, far = 1, 2, 4
        both = near ^ far
        send("a1", 0, near)
        send("a0", 0, far)
        send("a0", 0, near)
        send("a1", 0, far)
        for kind in kinds:
            send(kind, 0, core)
        for load in loads:
            load.start()
        square_columns()
        for mask in range(1, n):
            square_copy(mask).start()
        relay("a0", far)
        send("a0", far, near)
        send_across("a0", far)
        relay("a1", near)
        send("a1", near, far)
        send_across("a1", near)
        send("g1", 0, near)
        send("g0", 0, far)
        send("g0", 0, near)
        send("g1", 0, far)
        relay("a0", near)
        send_across("a0", near)
        relay("a1", far)
        send_across("a1", far)
        complete(core)
        add_slots((0, core), True, 0, capacity)
        add_selected((0, core), True)
        relay("a0", both)
        send_across("a0", both)
        relay("a1", both)
        send_across("a1", both)
        relay("z0", far)
        relay("z1", near)
        relay("z0", near)
        relay("g0", far)
        send("g0", far, near)
        relay("g1", near)
        send("g1", near, far)
        relay("z1", far)
        relay("g0", near)
        relay("g1", far)
        complete(near ^ core)
        complete(far ^ core)
        middle = (near, near ^ core, far, far ^ core)
        add_slots(middle, False, 0, capacity // 2)
        relay("z0", both)
        relay("z1", both)
        add_slots(middle, False, capacity // 2, capacity)
        add_selected(middle, False)
        relay("g0", both)
        relay("g1", both)
        complete(both ^ core)
    else:
        for mask in range(1, n):
            for kind in parts:
                send(kind, 0, mask)
        for load in loads:
            load.start()
        square_columns()
        for mask in range(1, n):
            square_copy(mask).start()
        add_slots((0,), True, 0, capacity)
        add_selected((0,), True)
        for mask in range(1, n):
            complete(mask)
            if mask not in late:
                add_slots((mask,), False, 0, capacity)
                add_selected((mask,), False)

    whole = squares[0]
    for mask in range(1, n):
        square_copy(mask).wait_recv()
        whole = whole + squares[mask]
    for tile in range(tiles_here):
        norm[:, pl.ds(tile * TILE, TILE)] = jnp.sqrt(whole[tile : tile + 1])
    for load in loads:
        load.wait()
    for copy in started:
        copy.wait_send()
    for mask in range(1, n):
        square_copy(mask).wait_send()


def update_kernel(late_count, group, *refs):
    held_a, held_g = refs[:late_count], refs[late_count : 2 * late_count]
    refs = refs[2 * late_count :]
    sel_states, (off_moment, off_second) = refs[:3], refs[3:5]
    total, sel_sum, norm, weight_source = refs[5:9]
    table_source = refs[9]
    sel_new, off_new, norm_new = refs[10:13], refs[13:16], refs[16]
    table, weights, stage, sel_stage, load_sem, stage_sem, sel_sem = refs[17:]
    me = lax.axis_index("dp")
    capacity, row_block = total.shape[:2]
    sel_count = sel_sum.shape[1] // TILE
    groups = capacity // group
    depth = weights.shape[0]
    rows_once = min(ROWS_ONCE, row_block)

    def load_of(at, ring):
        return pltpu.make_async_copy(
            weight_source.at[pl.ds(at * group, group)], weights.at[ring], load_sem.at[ring]
        )

    def out_of(which, at, ring):
        return pltpu.make_async_copy(
            stage.at[which, ring],
            off_new[which].at[pl.ds(at * group, group)],
            stage_sem.at[which, ring],
        )

    table_copy = pltpu.make_async_copy(table_source, table, sel_sem.at[4])
    table_copy.start()
    for at in range(min(depth, groups)):
        load_of(at, at).start()
    norm_copy = pltpu.make_async_copy(norm.at[0], norm_new, sel_sem.at[3])
    norm_copy.start()
    table_copy.wait()

    for i in range(sel_count):
        tile, place = table[3 * capacity + i], pl.ds(i * TILE, TILE)
        for row in range(0, row_block, rows_once):
            rows = pl.ds(row, rows_once)
            grad = sel_sum[rows, place]
            for a, g in zip(held_a, held_g):
                grad = grad + jnp.dot(
                    a[me, rows], g[tile], preferred_element_type=jnp.float32
                )
            news = adam_update(*(state[rows, place] for state in sel_states), grad)
            for which in range(3):
                sel_stage[which, rows, place] = news[which]
    sel_copies = [
        pltpu.make_async_copy(sel_stage.at[which], sel_new[which], sel_sem.at[which])
        for which in range(3)
    ]
    for copy in sel_copies:
        copy.start()

    @pl.loop(0, groups)
    def _(at):
        ring, turn = lax.rem(at, depth), lax.rem(at, 2)
        load_of(at, ring).wait()

        @pl.when(at >= 2)
        def _():
            for which in range(3):
                out_of(which, at, turn).wait()

        for k in range(group):
            slot = at * group + k
            block, tile = table[capacity + slot], table[slot]
            full = table[2 * capacity + slot] > 0
            for row in range(0, row_block, rows_once):
                rows = pl.ds(row, rows_once)
                value = total[slot, rows]
                for a, g in zip(held_a, held_g):
                    value = value + rounded(
                        jnp.dot(
                            a[block, rows], g[tile], preferred_element_type=jnp.float32
                        )
                    )
                grad = jnp.where(full, rounded(value), 0.0)
                news = adam_update(
                    weights[ring, k, rows],
                    off_moment[slot, rows],
                    off_second[slot, rows],
                    grad,
                )
                for which in range(3):
                    stage[which, turn, k, rows] = news[which]
        for which in range(3):
            out_of(which, at, turn).start()

        @pl.when(at + depth < groups)
        def _():
            load_of(at + depth, ring).start()

    for at in range(max(groups - 2, 0), groups):
        for which in range(3):
            out_of(which, at, at % 2).wait()
    for copy in sel_copies:
        copy.wait()
    norm_copy.wait()


def body(
    acts,
    grad_out,
    selected,
    owner,
    sel_weight,
    sel_moment,
    sel_second,
    off_weight,
    off_moment,
    off_second,
):
    n = lax.axis_size("dp")
    tokens_here, rows_all = acts.shape
    cols_here = grad_out.shape[1]
    tiles_here = cols_here // TILE
    sel_count = selected.shape[1]
    row_block = rows_all // n
    capacity = off_weight.shape[2]
    piece_count = owner.shape[1]
    paired = n == 8 and lax.axis_size("tensor") % 2 == 0
    late = (6, 7) if paired else (n - 1,)
    sel_states = (sel_weight, sel_moment, sel_second)
    slot_shape = (capacity, row_block, TILE)
    off_states = tuple(
        state.reshape(slot_shape) for state in (off_weight, off_moment, off_second)
    )
    in_vmem = pl.BlockSpec(memory_space=pltpu.VMEM)
    in_smem = pl.BlockSpec(memory_space=pltpu.SMEM)
    anywhere = pl.BlockSpec(memory_space=pltpu.HBM)
    a_shape, g_shape = (n, row_block, tokens_here), (tiles_here, tokens_here, TILE)
    table_shape = (3 * capacity + sel_count,)
    sel_shape = (row_block, sel_count * TILE)
    sends = 42 if paired else 2 * (n - 1)
    early_count = n - len(late)
    sel_row = selected.reshape(sel_count)
    half = jnp.dtype(jnp.bfloat16).itemsize
    gathered = (early_count + 1) * tokens_here * rows_all + early_count * tokens_here * cols_here
    gather_limit = half * gathered + 3 * MIB
    update_limit = gather_limit
    table = pl.pallas_call(
        functools.partial(table_kernel, n, capacity),
        name="tables",
        out_shape=jax.ShapeDtypeStruct(table_shape, jnp.int32),
        in_specs=[in_smem] * 2,
        out_specs=in_smem,
        scratch_shapes=[
            pltpu.SMEM((piece_count + 2,), jnp.int32),
            pltpu.SMEM((tiles_here + 1,), jnp.int32),
            pltpu.SMEM((tiles_here - sel_count,), jnp.int32),
        ],
    )(sel_row, owner.reshape(piece_count))
    outs = pl.pallas_call(
        functools.partial(gather_kernel, n, paired, late),
        name="gather",
        out_shape=[pltpu.VMEM(a_shape, jnp.bfloat16)] * len(late)
        + [pltpu.VMEM(g_shape, jnp.bfloat16)] * len(late)
        + [pltpu.VMEM(sel_shape, jnp.float32)] * 3
        + [pltpu.VMEM(slot_shape, jnp.float32)] * 2
        + [
            pltpu.VMEM(slot_shape, jnp.float32),
            pltpu.VMEM(sel_shape, jnp.float32),
            pltpu.VMEM((1, cols_here), jnp.float32),
        ],
        in_specs=[anywhere] * 8,
        out_specs=[in_vmem] * (2 * len(late) + 8),
        scratch_shapes=[
            pltpu.SMEM(table_shape, jnp.int32),
            pltpu.VMEM((tokens_here, rows_all), jnp.bfloat16),
            pltpu.VMEM((n, tiles_here, TILE), jnp.float32),
            pltpu.SemaphoreType.DMA((sends,)),
            pltpu.SemaphoreType.DMA((6 * (n - 1),)),
            pltpu.SemaphoreType.DMA((n - 1,)),
            pltpu.SemaphoreType.DMA((n - 1,)),
            pltpu.SemaphoreType.DMA((7,)),
            pltpu.SemaphoreType.DMA((tiles_here,)),
        ]
        + [pltpu.VMEM(a_shape, jnp.bfloat16)] * early_count
        + [pltpu.VMEM(g_shape, jnp.bfloat16)] * early_count,
        compiler_params=pltpu.CompilerParams(
            collective_id=0, has_side_effects=True, vmem_limit_bytes=gather_limit
        ),
    )(
        *(
            in_hbm(each)
            for each in (
                table,
                acts,
                grad_out,
                *sel_states,
                *off_states[1:],
            )
        )
    )
    lates, outs = outs[: 2 * len(late)], list(outs[2 * len(late) :])
    kept, (total, sel_sum, norm) = outs[:5], outs[5:]
    group = unroll_of(capacity)
    news = pl.pallas_call(
        functools.partial(update_kernel, len(late), group),
        name="update",
        out_shape=[jax.ShapeDtypeStruct(sel_shape, jnp.float32)] * 3
        + [jax.ShapeDtypeStruct(slot_shape, jnp.float32)] * 3
        + [jax.ShapeDtypeStruct((cols_here,), jnp.float32)],
        in_specs=[in_vmem] * (2 * len(late) + 8) + [anywhere] * 2,
        out_specs=[anywhere] * 7,
        scratch_shapes=[
            pltpu.SMEM(table_shape, jnp.int32),
            pltpu.VMEM((DEPTH, group, row_block, TILE), jnp.float32),
            pltpu.VMEM((3, 2, group, row_block, TILE), jnp.float32),
            pltpu.VMEM((3, *sel_shape), jnp.float32),
            pltpu.SemaphoreType.DMA((DEPTH,)),
            pltpu.SemaphoreType.DMA((3, 2)),
            pltpu.SemaphoreType.DMA((5,)),
        ],
        compiler_params=pltpu.CompilerParams(vmem_limit_bytes=update_limit),
    )(
        *lates,
        *kept,
        total,
        sel_sum,
        norm,
        in_hbm(off_states[0]),
        in_hbm(table),
    )
    return (
        news[6],
        *news[:3],
        *(new.reshape(off_weight.shape) for new in news[3:6]),
    )


def solution(mesh):
    placed = (
        P("dp", None),
        P("dp", "tensor"),
        P("tensor", None),
        P("tensor", None, None),
        P("dp", "tensor"),
        P("dp", "tensor"),
        P("dp", "tensor"),
        P("dp", "tensor", None, None, None),
        P("dp", "tensor", None, None, None),
        P("dp", "tensor", None, None, None),
    )
    return jax.shard_map(
        body,
        mesh=mesh,
        in_specs=placed,
        out_specs=(
            P("tensor"),
            P("dp", "tensor"),
            P("dp", "tensor"),
            P("dp", "tensor"),
            P("dp", "tensor", None, None, None),
            P("dp", "tensor", None, None, None),
            P("dp", "tensor", None, None, None),
        ),
        check_vma=False,
    )
```

```python
import functools

import jax
import jax.numpy as jnp
from jax import lax
from jax.experimental import pallas as pl
from jax.experimental.pallas import tpu as pltpu
from jax.sharding import PartitionSpec as P

TILE = 128
ROWS_ONCE = 128
MIB = 1024 * 1024

beta_one = 0.9
beta_two = 0.95
adam_eps = 1e-08
learn_rate = 0.01
decay_rate = 0.1
step_count = 10.0

MESH = pl.DeviceIdType.MESH


def adam_update(weight, moment, second, grad):
    first_fix = 1.0 - beta_one**step_count
    root_fix = (1.0 - beta_two**step_count) ** 0.5
    moment_new = beta_one * moment + (1.0 - beta_one) * grad
    second_new = beta_two * second + (1.0 - beta_two) * (grad * grad)
    inverse = lax.rsqrt(second_new)
    scale = second_new * inverse + adam_eps * root_fix
    inverse = inverse + inverse * (1.0 - scale * inverse)
    update = moment_new * (learn_rate * root_fix / first_fix) * inverse
    return weight * (1.0 - learn_rate * decay_rate) - update, moment_new, second_new


def flip_bits(index, mask):
    result, bit = index, 1
    while bit <= mask:
        if mask & bit:
            result = result + bit * (1 - 2 * ((index // bit) % 2))
        bit *= 2
    return result


def rounded(value):
    return value.astype(jnp.bfloat16).astype(jnp.float32)


def in_hbm(array):
    return pltpu.with_memory_space_constraint(array, pltpu.HBM)


def unroll_of(count):
    return next(k for k in (3, 2, 1) if count % k == 0)


def make_tables(
    n, capacity, sel_tile, owner, table, next_piece, next_free, rest_tile
):
    me = lax.axis_index("dp")
    sel_count = sel_tile.shape[0]
    piece_count, tiles_here = owner.shape[0], next_free.shape[0] - 1

    def piece_step(i, following):
        p = piece_count - 1 - i
        following = jnp.where(owner[p] == me, p, following)
        next_piece[p] = following
        return following

    next_piece[piece_count] = piece_count
    next_piece[piece_count + 1] = piece_count
    lax.fori_loop(0, piece_count, piece_step, jnp.int32(piece_count))

    def free_step(i, following):
        t = tiles_here - 1 - i
        taken = jnp.int32(0)
        for k in range(sel_count):
            taken = taken + (sel_tile[k] == t).astype(jnp.int32)
        following = jnp.where(taken == 0, t, following)
        next_free[t] = following
        return following

    next_free[tiles_here] = 0
    lax.fori_loop(0, tiles_here, free_step, jnp.int32(0))

    def rest_step(k, at):
        tile = next_free[at]
        rest_tile[k] = tile
        return tile + 1

    lax.fori_loop(0, tiles_here - sel_count, rest_step, jnp.int32(0))

    def slot_step(s, at):
        p = next_piece[at]
        found = p < piece_count
        piece = jnp.where(found, p, 0)
        table[s] = rest_tile[lax.div(piece, n)]
        table[capacity + s] = lax.rem(piece, n)
        table[2 * capacity + s] = found.astype(jnp.int32)
        return p + 1 - (p // piece_count)

    lax.fori_loop(0, capacity, slot_step, jnp.int32(0))
    for k in range(sel_count):
        table[3 * capacity + k] = sel_tile[k]


def gather_kernel(n, paired, late, selected, owners, acts, grad, *refs):
    states, refs = refs[:6], refs[6:]
    late_a, late_g = refs[: len(late)], refs[len(late) : 2 * len(late)]
    refs = refs[2 * len(late) :]
    kept = refs[:6]
    total, sel_sum, norm, table = refs[6:10]
    early = [mask for mask in range(n) if mask not in late]
    refs = refs[10:]
    raw, squares, sel_tile, owner, next_piece, next_free, rest_tile = refs[:7]
    send_sem, recv_sem, send_q, recv_q, load_sem, grad_sem = refs[7:13]
    held_a = dict(zip(early, refs[13 : 13 + len(early)])) | dict(zip(late, late_a))
    held_g = dict(zip(early, refs[13 + len(early) :])) | dict(zip(late, late_g))

    layer = lax.axis_index("tensor")
    me = lax.axis_index("dp")
    capacity = total.shape[0]
    sel_count = sel_sum.shape[1] // TILE
    row_block = total.shape[1]
    tiles_here = grad.shape[1] // TILE
    kinds = ("a0", "a1", "z0", "z1", "g0", "g1")
    if paired:
        side, part = layer % 2, n // 4
        cut = tiles_here // 2
        parts = {
            "a0": (held_a, (pl.ds(side * 2 * part, part),)),
            "a1": (held_a, (pl.ds(side * 2 * part + part, part),)),
            "z0": (held_a, (pl.ds((1 - side) * 2 * part, part),)),
            "z1": (held_a, (pl.ds((1 - side) * 2 * part + part, part),)),
            "g0": (held_g, (pl.ds(0, cut),)),
            "g1": (held_g, (pl.ds(cut, tiles_here - cut),)),
        }
    else:
        parts = {
            "a0": (held_a, (slice(None),)),
            "g0": (held_g, (slice(None),)),
        }

    own_acts = pltpu.make_async_copy(acts, raw, load_sem.at[0])
    own_tables = [pltpu.make_async_copy(owners, owner, load_sem.at[1])]
    if sel_count == 1:
        sel_tile[0] = selected[0]
    else:
        own_tables.append(pltpu.make_async_copy(selected, sel_tile, load_sem.at[2]))
    own_grads = [
        pltpu.make_async_copy(
            grad.at[:, pl.ds(tile * TILE, TILE)], held_g[0].at[tile], grad_sem.at[tile]
        )
        for tile in range(tiles_here)
    ]
    own_acts.start()
    for copy in own_tables:
        copy.start()
    for copy in own_grads:
        copy.start()
    loads = []
    for number, (source, target) in enumerate(zip(states, kept)):
        source = source.at[pl.ds(0, target.shape[0])]
        load = pltpu.make_async_copy(source, target, load_sem.at[3 + number])
        loads.append(load)

    barrier = pltpu.get_barrier_semaphore()
    for mask in range(1, n):
        pl.semaphore_signal(
            barrier, inc=1, device_id={"dp": flip_bits(me, mask)}, device_id_type=MESH
        )
    if paired:
        pl.semaphore_signal(
            barrier, inc=1, device_id={"tensor": flip_bits(layer, 1)}, device_id_type=MESH
        )
    own_acts.wait()
    for block in range(n):
        held_a[0][block] = raw[:, pl.ds(block * row_block, row_block)].T
    for copy in own_grads:
        copy.wait()
    pl.semaphore_wait(barrier, n if paired else n - 1)

    started = []

    def at_part(kind, mask):
        slots, place = parts[kind]
        return slots[mask].at[place]

    def recv_of(kind, mask):
        return recv_sem.at[kinds.index(kind) * (n - 1) + mask - 1]

    def copy_of(kind, mask, peer, number):
        there = mask ^ peer
        slots, place = parts[kind]
        return pltpu.make_async_remote_copy(
            src_ref=slots[mask].at[place],
            dst_ref=slots[there].at[place],
            send_sem=send_sem.at[number],
            recv_sem=recv_of(kind, there),
            device_id={"dp": flip_bits(me, peer)},
            device_id_type=MESH,
        )

    def send(kind, mask, peer):
        copy = copy_of(kind, mask, peer, len(started))
        copy.start()
        started.append(copy)

    def send_across(kind, mask):
        copy = pltpu.make_async_remote_copy(
            src_ref=at_part(kind, mask),
            dst_ref=at_part(kind, mask),
            send_sem=send_sem.at[len(started)],
            recv_sem=recv_of("z" + kind[1], mask),
            device_id={"tensor": flip_bits(layer, 1)},
            device_id_type=MESH,
        )
        copy.start()
        started.append(copy)

    def arrived(kind, mask):
        copy_of(kind, 0, mask, 0).wait_recv()

    def square_columns():
        whole = held_a[0][...].reshape(n * row_block, raw.shape[0])
        gram = jnp.dot(raw[...], whole, preferred_element_type=jnp.float32)
        high = gram.astype(jnp.bfloat16)
        rest = gram - high.astype(jnp.float32)
        middle = rest.astype(jnp.bfloat16)
        low = (rest - middle.astype(jnp.float32)).astype(jnp.bfloat16)

        @pl.loop(0, tiles_here, unroll=unroll_of(tiles_here))
        def _(tile):
            piece = held_g[0][tile]
            product = jnp.dot(low, piece, preferred_element_type=jnp.float32)
            product += jnp.dot(middle, piece, preferred_element_type=jnp.float32)
            product += jnp.dot(high, piece, preferred_element_type=jnp.float32)
            squares[0, pl.ds(tile, 1)] = jnp.sum(
                piece.astype(jnp.float32) * product, axis=0, keepdims=True
            )

    def square_copy(mask):
        return pltpu.make_async_remote_copy(
            src_ref=squares.at[0],
            dst_ref=squares.at[mask],
            send_sem=send_q.at[mask - 1],
            recv_sem=recv_q.at[mask - 1],
            device_id={"dp": flip_bits(me, mask)},
            device_id_type=MESH,
        )

    def add_slots(masks, first, begin, end):
        @pl.loop(begin, end, unroll=unroll_of(end - begin))
        def _(slot):
            block, tile = table[capacity + slot], table[slot]
            value = None if first else total[slot]
            for mask in masks:
                partial = rounded(
                    jnp.dot(
                        held_a[mask][block],
                        held_g[mask][tile],
                        preferred_element_type=jnp.float32,
                    )
                )
                value = partial if value is None else value + partial
            total[slot] = value

    def add_selected(masks, first):
        for i in range(sel_count):
            tile, place = table[3 * capacity + i], pl.ds(i * TILE, TILE)
            value = None if first else sel_sum[:, place]
            for mask in masks:
                partial = jnp.dot(
                    held_a[mask][me],
                    held_g[mask][tile],
                    preferred_element_type=jnp.float32,
                )
                value = partial if value is None else value + partial
            sel_sum[:, place] = value

    def complete(mask, only=kinds):
        for kind in only:
            if kind in parts:
                arrived(kind, mask)

    def relay(kind, mask):
        arrived(kind, mask)
        send(kind, mask, 1)

    if paired:
        core, near, far = 1, 2, 4
        both = near ^ far
        send("a1", 0, near)
        send("a0", 0, far)
        send("a0", 0, near)
        send("a1", 0, far)
        for kind in kinds:
            send(kind, 0, core)
        for load in loads:
            load.start()
        for copy in own_tables:
            copy.wait()
        make_tables(n, capacity, sel_tile, owner, table, next_piece, next_free, rest_tile)
        square_columns()
        for mask in range(1, n):
            square_copy(mask).start()
        relay("a0", far)
        send("a0", far, near)
        send_across("a0", far)
        relay("a1", near)
        send("a1", near, far)
        send_across("a1", near)
        send("g1", 0, near)
        send("g0", 0, far)
        send("g0", 0, near)
        send("g1", 0, far)
        relay("a0", near)
        send_across("a0", near)
        relay("a1", far)
        send_across("a1", far)
        complete(core)
        add_slots((0, core), True, 0, capacity)
        add_selected((0, core), True)
        relay("a0", both)
        send_across("a0", both)
        relay("a1", both)
        send_across("a1", both)
        relay("z0", far)
        relay("z1", near)
        relay("z0", near)
        relay("g0", far)
        send("g0", far, near)
        relay("g1", near)
        send("g1", near, far)
        relay("z1", far)
        relay("g0", near)
        relay("g1", far)
        complete(near ^ core)
        complete(far ^ core)
        middle = (near, near ^ core, far, far ^ core)
        add_slots(middle, False, 0, capacity // 2)
        relay("z0", both)
        relay("z1", both)
        add_slots(middle, False, capacity // 2, capacity)
        add_selected(middle, False)
        relay("g0", both)
        relay("g1", both)
        complete(both ^ core)
    else:
        for mask in range(1, n):
            for kind in parts:
                send(kind, 0, mask)
        for load in loads:
            load.start()
        for copy in own_tables:
            copy.wait()
        make_tables(n, capacity, sel_tile, owner, table, next_piece, next_free, rest_tile)
        square_columns()
        for mask in range(1, n):
            square_copy(mask).start()
        add_slots((0,), True, 0, capacity)
        add_selected((0,), True)
        for mask in range(1, n):
            complete(mask)
            if mask not in late:
                add_slots((mask,), False, 0, capacity)
                add_selected((mask,), False)

    whole = squares[0]
    for mask in range(1, n):
        square_copy(mask).wait_recv()
        whole = whole + squares[mask]
    for tile in range(tiles_here):
        norm[:, pl.ds(tile * TILE, TILE)] = jnp.sqrt(whole[tile : tile + 1])
    for load in loads:
        load.wait()
    for copy in started:
        copy.wait_send()
    for mask in range(1, n):
        square_copy(mask).wait_send()


def update_kernel(late_count, group, *refs):
    held_a, held_g = refs[:late_count], refs[late_count : 2 * late_count]
    refs = refs[2 * late_count :]
    sel_states, (off_moment, off_second, ready) = refs[:3], refs[3:6]
    total, sel_sum, norm, weight_source, table = refs[6:11]
    sel_new, off_new, norm_new = refs[11:14], refs[14:17], refs[17]
    later, stage, sel_stage, load_sem, stage_sem, sel_sem = refs[18:]
    me = lax.axis_index("dp")
    capacity, row_block = total.shape[:2]
    sel_count = sel_sum.shape[1] // TILE
    groups = capacity // group
    begun = ready.shape[0] // group
    rows_once = min(ROWS_ONCE, row_block)

    load = pltpu.make_async_copy(
        weight_source.at[pl.ds(begun * group, later.shape[0])], later, load_sem.at[0]
    )

    def out_of(which, at, ring):
        return pltpu.make_async_copy(
            stage.at[which, ring],
            off_new[which].at[pl.ds(at * group, group)],
            stage_sem.at[which, ring],
        )

    load.start()
    norm_copy = pltpu.make_async_copy(norm.at[0], norm_new, sel_sem.at[3])
    norm_copy.start()

    for i in range(sel_count):
        tile, place = table[3 * capacity + i], pl.ds(i * TILE, TILE)
        for row in range(0, row_block, rows_once):
            rows = pl.ds(row, rows_once)
            grad = sel_sum[rows, place]
            for a, g in zip(held_a, held_g):
                grad = grad + jnp.dot(
                    a[me, rows], g[tile], preferred_element_type=jnp.float32
                )
            news = adam_update(*(state[rows, place] for state in sel_states), grad)
            for which in range(3):
                sel_stage[which, rows, place] = news[which]
    sel_copies = [
        pltpu.make_async_copy(sel_stage.at[which], sel_new[which], sel_sem.at[which])
        for which in range(3)
    ]
    for copy in sel_copies:
        copy.start()

    def update_group(at, weights, shift):
        turn = lax.rem(at, 2)

        @pl.when(at >= 2)
        def _():
            for which in range(3):
                out_of(which, at, turn).wait()

        for k in range(group):
            slot = at * group + k
            block, tile = table[capacity + slot], table[slot]
            full = table[2 * capacity + slot] > 0
            for row in range(0, row_block, rows_once):
                rows = pl.ds(row, rows_once)
                value = total[slot, rows]
                for a, g in zip(held_a, held_g):
                    value = value + rounded(
                        jnp.dot(
                            a[block, rows], g[tile], preferred_element_type=jnp.float32
                        )
                    )
                grad = jnp.where(full, rounded(value), 0.0)
                news = adam_update(
                    weights[slot - shift, rows],
                    off_moment[slot, rows],
                    off_second[slot, rows],
                    grad,
                )
                for which in range(3):
                    stage[which, turn, k, rows] = news[which]
        for which in range(3):
            out_of(which, at, turn).start()

    @pl.loop(0, begun)
    def _(at):
        update_group(at, ready, 0)

    load.wait()

    @pl.loop(begun, groups)
    def _(at):
        update_group(at, later, begun * group)

    for at in range(max(groups - 2, 0), groups):
        for which in range(3):
            out_of(which, at, at % 2).wait()
    for copy in sel_copies:
        copy.wait()
    norm_copy.wait()


def body(
    acts,
    grad_out,
    selected,
    owner,
    sel_weight,
    sel_moment,
    sel_second,
    off_weight,
    off_moment,
    off_second,
):
    n = lax.axis_size("dp")
    tokens_here, rows_all = acts.shape
    cols_here = grad_out.shape[1]
    tiles_here = cols_here // TILE
    sel_count = selected.shape[1]
    row_block = rows_all // n
    capacity = off_weight.shape[2]
    piece_count = owner.shape[1]
    paired = n == 8 and lax.axis_size("tensor") % 2 == 0
    late = (6, 7) if paired else (n - 1,)
    sel_states = (sel_weight, sel_moment, sel_second)
    slot_shape = (capacity, row_block, TILE)
    off_states = tuple(
        state.reshape(slot_shape) for state in (off_weight, off_moment, off_second)
    )
    in_vmem = pl.BlockSpec(memory_space=pltpu.VMEM)
    in_smem = pl.BlockSpec(memory_space=pltpu.SMEM)
    anywhere = pl.BlockSpec(memory_space=pltpu.HBM)
    a_shape, g_shape = (n, row_block, tokens_here), (tiles_here, tokens_here, TILE)
    table_shape = (3 * capacity + sel_count,)
    sel_shape = (row_block, sel_count * TILE)
    sends = 42 if paired else 2 * (n - 1)
    early_count = n - len(late)
    sel_row = selected.reshape(sel_count)
    group = unroll_of(capacity)
    ready = capacity // group * 2 // 3 * group
    half = jnp.dtype(jnp.bfloat16).itemsize
    gathered = (early_count + 1) * tokens_here * rows_all + early_count * tokens_here * cols_here
    gather_limit = half * gathered + MIB // 2
    update_limit = gather_limit
    outs = pl.pallas_call(
        functools.partial(gather_kernel, n, paired, late),
        name="gather",
        out_shape=[pltpu.VMEM(a_shape, jnp.bfloat16)] * len(late)
        + [pltpu.VMEM(g_shape, jnp.bfloat16)] * len(late)
        + [pltpu.VMEM(sel_shape, jnp.float32)] * 3
        + [pltpu.VMEM(slot_shape, jnp.float32)] * 2
        + [
            pltpu.VMEM((ready, row_block, TILE), jnp.float32),
            pltpu.VMEM(slot_shape, jnp.float32),
            pltpu.VMEM(sel_shape, jnp.float32),
            pltpu.VMEM((1, cols_here), jnp.float32),
            jax.ShapeDtypeStruct(table_shape, jnp.int32),
        ],
        in_specs=[in_smem if sel_count == 1 else anywhere] + [anywhere] * 9,
        out_specs=[in_vmem] * (2 * len(late) + 9) + [in_smem],
        scratch_shapes=[
            pltpu.VMEM((tokens_here, rows_all), jnp.bfloat16),
            pltpu.VMEM((n, tiles_here, TILE), jnp.float32),
            pltpu.SMEM((sel_count,), jnp.int32),
            pltpu.SMEM((piece_count,), jnp.int32),
            pltpu.SMEM((piece_count + 2,), jnp.int32),
            pltpu.SMEM((tiles_here + 1,), jnp.int32),
            pltpu.SMEM((tiles_here - sel_count,), jnp.int32),
            pltpu.SemaphoreType.DMA((sends,)),
            pltpu.SemaphoreType.DMA((6 * (n - 1),)),
            pltpu.SemaphoreType.DMA((n - 1,)),
            pltpu.SemaphoreType.DMA((n - 1,)),
            pltpu.SemaphoreType.DMA((9,)),
            pltpu.SemaphoreType.DMA((tiles_here,)),
        ]
        + [pltpu.VMEM(a_shape, jnp.bfloat16)] * early_count
        + [pltpu.VMEM(g_shape, jnp.bfloat16)] * early_count,
        compiler_params=pltpu.CompilerParams(
            collective_id=0, has_side_effects=True, vmem_limit_bytes=gather_limit
        ),
    )(
        sel_row if sel_count == 1 else in_hbm(sel_row),
        *(
            in_hbm(each)
            for each in (
                owner.reshape(piece_count),
                acts,
                grad_out,
                *sel_states,
                *off_states[1:],
                off_states[0],
            )
        )
    )
    lates, outs = outs[: 2 * len(late)], list(outs[2 * len(late) :])
    kept, (total, sel_sum, norm, table) = outs[:6], outs[6:]
    news = pl.pallas_call(
        functools.partial(update_kernel, len(late), group),
        name="update",
        out_shape=[jax.ShapeDtypeStruct(sel_shape, jnp.float32)] * 3
        + [jax.ShapeDtypeStruct(slot_shape, jnp.float32)] * 3
        + [jax.ShapeDtypeStruct((cols_here,), jnp.float32)],
        in_specs=[in_vmem] * (2 * len(late) + 9) + [anywhere, in_smem],
        out_specs=[anywhere] * 7,
        scratch_shapes=[
            pltpu.VMEM((capacity - ready, row_block, TILE), jnp.float32),
            pltpu.VMEM((3, 2, group, row_block, TILE), jnp.float32),
            pltpu.VMEM((3, *sel_shape), jnp.float32),
            pltpu.SemaphoreType.DMA((1,)),
            pltpu.SemaphoreType.DMA((3, 2)),
            pltpu.SemaphoreType.DMA((4,)),
        ],
        compiler_params=pltpu.CompilerParams(vmem_limit_bytes=update_limit),
    )(
        *lates,
        *kept,
        total,
        sel_sum,
        norm,
        in_hbm(off_states[0]),
        table,
    )
    return (
        news[6],
        *news[:3],
        *(new.reshape(off_weight.shape) for new in news[3:6]),
    )


def solution(mesh):
    placed = (
        P("dp", None),
        P("dp", "tensor"),
        P("tensor", None),
        P("tensor", None, None),
        P("dp", "tensor"),
        P("dp", "tensor"),
        P("dp", "tensor"),
        P("dp", "tensor", None, None, None),
        P("dp", "tensor", None, None, None),
        P("dp", "tensor", None, None, None),
    )
    return jax.shard_map(
        body,
        mesh=mesh,
        in_specs=placed,
        out_specs=(
            P("tensor"),
            P("dp", "tensor"),
            P("dp", "tensor"),
            P("dp", "tensor"),
            P("dp", "tensor", None, None, None),
            P("dp", "tensor", None, None, None),
            P("dp", "tensor", None, None, None),
        ),
        check_vma=False,
    )
```

```python
import functools

import jax
import jax.numpy as jnp
from jax import lax
from jax.experimental import pallas as pl
from jax.experimental.pallas import tpu as pltpu
from jax.sharding import PartitionSpec as P

TILE = 128
ROWS_ONCE = 128
MIB = 1024 * 1024

beta_one = 0.9
beta_two = 0.95
adam_eps = 1e-08
learn_rate = 0.01
decay_rate = 0.1
step_count = 10.0

MESH = pl.DeviceIdType.MESH


def adam_update(weight, moment, second, grad):
    first_fix = 1.0 - beta_one**step_count
    root_fix = (1.0 - beta_two**step_count) ** 0.5
    moment_new = beta_one * moment + (1.0 - beta_one) * grad
    second_new = beta_two * second + (1.0 - beta_two) * (grad * grad)
    inverse = lax.rsqrt(second_new)
    scale = second_new * inverse + adam_eps * root_fix
    inverse = inverse + inverse * (1.0 - scale * inverse)
    update = moment_new * (learn_rate * root_fix / first_fix) * inverse
    return weight * (1.0 - learn_rate * decay_rate) - update, moment_new, second_new


def flip_bits(index, mask):
    result, bit = index, 1
    while bit <= mask:
        if mask & bit:
            result = result + bit * (1 - 2 * ((index // bit) % 2))
        bit *= 2
    return result


def rounded(value):
    return value.astype(jnp.bfloat16).astype(jnp.float32)


def in_hbm(array):
    return pltpu.with_memory_space_constraint(array, pltpu.HBM)


def unroll_of(count):
    return next(k for k in (3, 2, 1) if count % k == 0)


def make_tables(
    n, capacity, sel_tile, owner, table, next_piece, next_free, rest_tile
):
    me = lax.axis_index("dp")
    sel_count = sel_tile.shape[0]
    piece_count, tiles_here = owner.shape[0], next_free.shape[0] - 1

    def piece_step(i, following):
        p = piece_count - 1 - i
        following = jnp.where(owner[p] == me, p, following)
        next_piece[p] = following
        return following

    next_piece[piece_count] = piece_count
    next_piece[piece_count + 1] = piece_count
    lax.fori_loop(0, piece_count, piece_step, jnp.int32(piece_count))

    def free_step(i, following):
        t = tiles_here - 1 - i
        taken = jnp.int32(0)
        for k in range(sel_count):
            taken = taken + (sel_tile[k] == t).astype(jnp.int32)
        following = jnp.where(taken == 0, t, following)
        next_free[t] = following
        return following

    next_free[tiles_here] = 0
    lax.fori_loop(0, tiles_here, free_step, jnp.int32(0))

    def rest_step(k, at):
        tile = next_free[at]
        rest_tile[k] = tile
        return tile + 1

    lax.fori_loop(0, tiles_here - sel_count, rest_step, jnp.int32(0))

    def slot_step(s, at):
        p = next_piece[at]
        found = p < piece_count
        piece = jnp.where(found, p, 0)
        table[s] = rest_tile[lax.div(piece, n)]
        table[capacity + s] = lax.rem(piece, n)
        table[2 * capacity + s] = found.astype(jnp.int32)
        return p + 1 - (p // piece_count)

    lax.fori_loop(0, capacity, slot_step, jnp.int32(0))
    for k in range(sel_count):
        table[3 * capacity + k] = sel_tile[k]


def gather_kernel(n, paired, late, selected, owners, acts, grad, *refs):
    states, refs = refs[:6], refs[6:]
    late_a, late_g = refs[: len(late)], refs[len(late) : 2 * len(late)]
    refs = refs[2 * len(late) :]
    kept = refs[:6]
    total, sel_sum, norm, table = refs[6:10]
    early = [mask for mask in range(n) if mask not in late]
    refs = refs[10:]
    raw, squares, sel_tile, owner, next_piece, next_free, rest_tile = refs[:7]
    send_sem, recv_sem, send_q, recv_q, load_sem, grad_sem = refs[7:13]
    held_a = dict(zip(early, refs[13 : 13 + len(early)])) | dict(zip(late, late_a))
    held_g = dict(zip(early, refs[13 + len(early) :])) | dict(zip(late, late_g))

    layer = lax.axis_index("tensor")
    me = lax.axis_index("dp")
    capacity = total.shape[0]
    sel_count = sel_sum.shape[1] // TILE
    row_block = total.shape[1]
    tiles_here = grad.shape[1] // TILE
    kinds = ("a0", "a1", "z0", "z1", "s0", "g0", "g1")
    if paired:
        side, part = layer % 2, n // 4
        first, cut = tiles_here // 7, tiles_here // 2
        parts = {
            "a0": (held_a, (pl.ds(side * 2 * part, part),)),
            "a1": (held_a, (pl.ds(side * 2 * part + part, part),)),
            "z0": (held_a, (pl.ds((1 - side) * 2 * part, part),)),
            "z1": (held_a, (pl.ds((1 - side) * 2 * part + part, part),)),
            "s0": (held_g, (pl.ds(0, first),)),
            "g0": (held_g, (pl.ds(first, cut - first),)),
            "g1": (held_g, (pl.ds(cut, tiles_here - cut),)),
        }
    else:
        parts = {
            "a0": (held_a, (slice(None),)),
            "g0": (held_g, (slice(None),)),
        }

    own_acts = pltpu.make_async_copy(acts, raw, load_sem.at[0])
    own_tables = [pltpu.make_async_copy(owners, owner, load_sem.at[1])]
    if sel_count == 1:
        sel_tile[0] = selected[0]
    else:
        own_tables.append(pltpu.make_async_copy(selected, sel_tile, load_sem.at[2]))
    own_grads = [
        pltpu.make_async_copy(
            grad.at[:, pl.ds(tile * TILE, TILE)], held_g[0].at[tile], grad_sem.at[tile]
        )
        for tile in range(tiles_here)
    ]
    own_acts.start()
    for copy in own_tables:
        copy.start()
    for copy in own_grads:
        copy.start()
    loads = []
    for number, (source, target) in enumerate(zip(states, kept)):
        source = source.at[pl.ds(0, target.shape[0])]
        load = pltpu.make_async_copy(source, target, load_sem.at[3 + number])
        loads.append(load)

    barrier = pltpu.get_barrier_semaphore()
    for mask in range(1, n):
        pl.semaphore_signal(
            barrier, inc=1, device_id={"dp": flip_bits(me, mask)}, device_id_type=MESH
        )
    if paired:
        pl.semaphore_signal(
            barrier, inc=1, device_id={"tensor": flip_bits(layer, 1)}, device_id_type=MESH
        )
    for copy in own_grads:
        copy.wait()
    pl.semaphore_wait(barrier, n if paired else n - 1)

    started = []

    def at_part(kind, mask):
        slots, place = parts[kind]
        return slots[mask].at[place]

    def recv_of(kind, mask):
        return recv_sem.at[kinds.index(kind) * (n - 1) + mask - 1]

    def copy_of(kind, mask, peer, number):
        there = mask ^ peer
        slots, place = parts[kind]
        return pltpu.make_async_remote_copy(
            src_ref=slots[mask].at[place],
            dst_ref=slots[there].at[place],
            send_sem=send_sem.at[number],
            recv_sem=recv_of(kind, there),
            device_id={"dp": flip_bits(me, peer)},
            device_id_type=MESH,
        )

    def send(kind, mask, peer):
        copy = copy_of(kind, mask, peer, len(started))
        copy.start()
        started.append(copy)

    def send_across(kind, mask):
        copy = pltpu.make_async_remote_copy(
            src_ref=at_part(kind, mask),
            dst_ref=at_part(kind, mask),
            send_sem=send_sem.at[len(started)],
            recv_sem=recv_of("z" + kind[1], mask),
            device_id={"tensor": flip_bits(layer, 1)},
            device_id_type=MESH,
        )
        copy.start()
        started.append(copy)

    def arrived(kind, mask):
        copy_of(kind, 0, mask, 0).wait_recv()

    def square_columns():
        whole = held_a[0][...].reshape(n * row_block, raw.shape[0])
        gram = jnp.dot(raw[...], whole, preferred_element_type=jnp.float32)
        high = gram.astype(jnp.bfloat16)
        rest = gram - high.astype(jnp.float32)
        middle = rest.astype(jnp.bfloat16)
        low = (rest - middle.astype(jnp.float32)).astype(jnp.bfloat16)

        @pl.loop(0, tiles_here, unroll=unroll_of(tiles_here))
        def _(tile):
            piece = held_g[0][tile]
            product = jnp.dot(low, piece, preferred_element_type=jnp.float32)
            product += jnp.dot(middle, piece, preferred_element_type=jnp.float32)
            product += jnp.dot(high, piece, preferred_element_type=jnp.float32)
            squares[0, pl.ds(tile, 1)] = jnp.sum(
                piece.astype(jnp.float32) * product, axis=0, keepdims=True
            )

    def square_copy(mask):
        return pltpu.make_async_remote_copy(
            src_ref=squares.at[0],
            dst_ref=squares.at[mask],
            send_sem=send_q.at[mask - 1],
            recv_sem=recv_q.at[mask - 1],
            device_id={"dp": flip_bits(me, mask)},
            device_id_type=MESH,
        )

    def add_slots(masks, first, begin, end):
        @pl.loop(begin, end, unroll=unroll_of(end - begin))
        def _(slot):
            block, tile = table[capacity + slot], table[slot]
            value = None if first else total[slot]
            for mask in masks:
                partial = rounded(
                    jnp.dot(
                        held_a[mask][block],
                        held_g[mask][tile],
                        preferred_element_type=jnp.float32,
                    )
                )
                value = partial if value is None else value + partial
            total[slot] = value

    def add_selected(masks, first):
        for i in range(sel_count):
            tile, place = table[3 * capacity + i], pl.ds(i * TILE, TILE)
            value = None if first else sel_sum[:, place]
            for mask in masks:
                partial = jnp.dot(
                    held_a[mask][me],
                    held_g[mask][tile],
                    preferred_element_type=jnp.float32,
                )
                value = partial if value is None else value + partial
            sel_sum[:, place] = value

    def complete(mask, only=kinds):
        for kind in only:
            if kind in parts:
                arrived(kind, mask)

    def relay(kind, mask):
        arrived(kind, mask)
        send(kind, mask, 1)

    def turn_acts():
        own_acts.wait()
        for block in range(n):
            held_a[0][block] = raw[:, pl.ds(block * row_block, row_block)].T

    if paired:
        core, near, far = 1, 2, 4
        both = near ^ far
        send("s0", 0, near)
        send("s0", 0, far)
        turn_acts()
        send("a1", 0, near)
        send("a0", 0, far)
        send("a0", 0, near)
        send("a1", 0, far)
        for kind in kinds:
            send(kind, 0, core)
        for load in loads:
            load.start()
        relay("a0", far)
        send("a0", far, near)
        send_across("a0", far)
        relay("a1", near)
        send("a1", near, far)
        send_across("a1", near)
        send("g1", 0, near)
        send("g0", 0, far)
        send("g0", 0, near)
        send("g1", 0, far)
        square_columns()
        for mask in range(1, n):
            square_copy(mask).start()
        relay("a0", near)
        send_across("a0", near)
        relay("a1", far)
        send_across("a1", far)
        for copy in own_tables:
            copy.wait()
        make_tables(n, capacity, sel_tile, owner, table, next_piece, next_free, rest_tile)
        relay("a0", both)
        send_across("a0", both)
        relay("a1", both)
        send_across("a1", both)
        complete(core)
        add_slots((0, core), True, 0, capacity)
        add_selected((0, core), True)
        relay("s0", far)
        send("s0", far, near)
        relay("s0", near)
        relay("z0", far)
        relay("z1", near)
        relay("z0", near)
        relay("g0", far)
        send("g0", far, near)
        relay("g1", near)
        send("g1", near, far)
        relay("z1", far)
        relay("g0", near)
        relay("g1", far)
        complete(near ^ core)
        complete(far ^ core)
        middle = (near, near ^ core, far, far ^ core)
        add_slots(middle, False, 0, capacity // 2)
        relay("z0", both)
        relay("z1", both)
        add_slots(middle, False, capacity // 2, capacity)
        add_selected(middle, False)
        relay("s0", both)
        relay("g0", both)
        relay("g1", both)
        complete(both ^ core)
    else:
        turn_acts()
        for mask in range(1, n):
            for kind in parts:
                send(kind, 0, mask)
        for load in loads:
            load.start()
        for copy in own_tables:
            copy.wait()
        make_tables(n, capacity, sel_tile, owner, table, next_piece, next_free, rest_tile)
        square_columns()
        for mask in range(1, n):
            square_copy(mask).start()
        add_slots((0,), True, 0, capacity)
        add_selected((0,), True)
        for mask in range(1, n):
            complete(mask)
            if mask not in late:
                add_slots((mask,), False, 0, capacity)
                add_selected((mask,), False)

    whole = squares[0]
    for mask in range(1, n):
        square_copy(mask).wait_recv()
        whole = whole + squares[mask]
    for tile in range(tiles_here):
        norm[:, pl.ds(tile * TILE, TILE)] = jnp.sqrt(whole[tile : tile + 1])
    for load in loads:
        load.wait()
    for copy in started:
        copy.wait_send()
    for mask in range(1, n):
        square_copy(mask).wait_send()


def update_kernel(late_count, group, *refs):
    held_a, held_g = refs[:late_count], refs[late_count : 2 * late_count]
    refs = refs[2 * late_count :]
    sel_states, (off_moment, off_second, ready) = refs[:3], refs[3:6]
    total, sel_sum, norm, weight_source, table = refs[6:11]
    sel_new, off_new, norm_new = refs[11:14], refs[14:17], refs[17]
    later, stage, sel_stage, load_sem, stage_sem, sel_sem = refs[18:]
    me = lax.axis_index("dp")
    capacity, row_block = total.shape[:2]
    sel_count = sel_sum.shape[1] // TILE
    groups = capacity // group
    begun = ready.shape[0] // group
    rows_once = min(ROWS_ONCE, row_block)

    load = pltpu.make_async_copy(
        weight_source.at[pl.ds(begun * group, later.shape[0])], later, load_sem.at[0]
    )

    def out_of(which, at, ring):
        return pltpu.make_async_copy(
            stage.at[which, ring],
            off_new[which].at[pl.ds(at * group, group)],
            stage_sem.at[which, ring],
        )

    load.start()
    norm_copy = pltpu.make_async_copy(norm.at[0], norm_new, sel_sem.at[3])
    norm_copy.start()

    for i in range(sel_count):
        tile, place = table[3 * capacity + i], pl.ds(i * TILE, TILE)
        for row in range(0, row_block, rows_once):
            rows = pl.ds(row, rows_once)
            grad = sel_sum[rows, place]
            for a, g in zip(held_a, held_g):
                grad = grad + jnp.dot(
                    a[me, rows], g[tile], preferred_element_type=jnp.float32
                )
            news = adam_update(*(state[rows, place] for state in sel_states), grad)
            for which in range(3):
                sel_stage[which, rows, place] = news[which]
    sel_copies = [
        pltpu.make_async_copy(sel_stage.at[which], sel_new[which], sel_sem.at[which])
        for which in range(3)
    ]
    for copy in sel_copies:
        copy.start()

    def update_group(at, weights, shift):
        turn = lax.rem(at, 4)

        @pl.when(at >= 4)
        def _():
            for which in range(3):
                out_of(which, at, turn).wait()

        for k in range(group):
            slot = at * group + k
            block, tile = table[capacity + slot], table[slot]
            full = table[2 * capacity + slot] > 0
            for row in range(0, row_block, rows_once):
                rows = pl.ds(row, rows_once)
                value = total[slot, rows]
                for a, g in zip(held_a, held_g):
                    value = value + rounded(
                        jnp.dot(
                            a[block, rows], g[tile], preferred_element_type=jnp.float32
                        )
                    )
                grad = jnp.where(full, rounded(value), 0.0)
                news = adam_update(
                    weights[slot - shift, rows],
                    off_moment[slot, rows],
                    off_second[slot, rows],
                    grad,
                )
                for which in range(3):
                    stage[which, turn, k, rows] = news[which]
        for which in range(3):
            out_of(which, at, turn).start()

    @pl.loop(0, begun)
    def _(at):
        update_group(at, ready, 0)

    load.wait()

    @pl.loop(begun, groups)
    def _(at):
        update_group(at, later, begun * group)

    for at in range(max(groups - 4, 0), groups):
        for which in range(3):
            out_of(which, at, at % 4).wait()
    for copy in sel_copies:
        copy.wait()
    norm_copy.wait()


def body(
    acts,
    grad_out,
    selected,
    owner,
    sel_weight,
    sel_moment,
    sel_second,
    off_weight,
    off_moment,
    off_second,
):
    n = lax.axis_size("dp")
    tokens_here, rows_all = acts.shape
    cols_here = grad_out.shape[1]
    tiles_here = cols_here // TILE
    sel_count = selected.shape[1]
    row_block = rows_all // n
    capacity = off_weight.shape[2]
    piece_count = owner.shape[1]
    paired = n == 8 and lax.axis_size("tensor") % 2 == 0
    late = (6, 7) if paired else (n - 1,)
    sel_states = (sel_weight, sel_moment, sel_second)
    slot_shape = (capacity, row_block, TILE)
    off_states = tuple(
        state.reshape(slot_shape) for state in (off_weight, off_moment, off_second)
    )
    in_vmem = pl.BlockSpec(memory_space=pltpu.VMEM)
    in_smem = pl.BlockSpec(memory_space=pltpu.SMEM)
    anywhere = pl.BlockSpec(memory_space=pltpu.HBM)
    a_shape, g_shape = (n, row_block, tokens_here), (tiles_here, tokens_here, TILE)
    table_shape = (3 * capacity + sel_count,)
    sel_shape = (row_block, sel_count * TILE)
    sends = 49 if paired else 2 * (n - 1)
    early_count = n - len(late)
    sel_row = selected.reshape(sel_count)
    group = 2 if capacity % 2 == 0 else 1
    ready = capacity // group * 2 // 3 * group
    half = jnp.dtype(jnp.bfloat16).itemsize
    gathered = (early_count + 1) * tokens_here * rows_all + early_count * tokens_here * cols_here
    gather_limit = half * gathered + MIB // 2
    update_limit = gather_limit
    outs = pl.pallas_call(
        functools.partial(gather_kernel, n, paired, late),
        name="gather",
        out_shape=[pltpu.VMEM(a_shape, jnp.bfloat16)] * len(late)
        + [pltpu.VMEM(g_shape, jnp.bfloat16)] * len(late)
        + [pltpu.VMEM(sel_shape, jnp.float32)] * 3
        + [pltpu.VMEM(slot_shape, jnp.float32)] * 2
        + [
            pltpu.VMEM((ready, row_block, TILE), jnp.float32),
            pltpu.VMEM(slot_shape, jnp.float32),
            pltpu.VMEM(sel_shape, jnp.float32),
            pltpu.VMEM((1, cols_here), jnp.float32),
            jax.ShapeDtypeStruct(table_shape, jnp.int32),
        ],
        in_specs=[in_smem if sel_count == 1 else anywhere] + [anywhere] * 9,
        out_specs=[in_vmem] * (2 * len(late) + 9) + [in_smem],
        scratch_shapes=[
            pltpu.VMEM((tokens_here, rows_all), jnp.bfloat16),
            pltpu.VMEM((n, tiles_here, TILE), jnp.float32),
            pltpu.SMEM((sel_count,), jnp.int32),
            pltpu.SMEM((piece_count,), jnp.int32),
            pltpu.SMEM((piece_count + 2,), jnp.int32),
            pltpu.SMEM((tiles_here + 1,), jnp.int32),
            pltpu.SMEM((tiles_here - sel_count,), jnp.int32),
            pltpu.SemaphoreType.DMA((sends,)),
            pltpu.SemaphoreType.DMA((7 * (n - 1),)),
            pltpu.SemaphoreType.DMA((n - 1,)),
            pltpu.SemaphoreType.DMA((n - 1,)),
            pltpu.SemaphoreType.DMA((9,)),
            pltpu.SemaphoreType.DMA((tiles_here,)),
        ]
        + [pltpu.VMEM(a_shape, jnp.bfloat16)] * early_count
        + [pltpu.VMEM(g_shape, jnp.bfloat16)] * early_count,
        compiler_params=pltpu.CompilerParams(
            collective_id=0, has_side_effects=True, vmem_limit_bytes=gather_limit
        ),
    )(
        sel_row if sel_count == 1 else in_hbm(sel_row),
        *(
            in_hbm(each)
            for each in (
                owner.reshape(piece_count),
                acts,
                grad_out,
                *sel_states,
                *off_states[1:],
                off_states[0],
            )
        )
    )
    lates, outs = outs[: 2 * len(late)], list(outs[2 * len(late) :])
    kept, (total, sel_sum, norm, table) = outs[:6], outs[6:]
    news = pl.pallas_call(
        functools.partial(update_kernel, len(late), group),
        name="update",
        out_shape=[jax.ShapeDtypeStruct(sel_shape, jnp.float32)] * 3
        + [jax.ShapeDtypeStruct(slot_shape, jnp.float32)] * 3
        + [jax.ShapeDtypeStruct((cols_here,), jnp.float32)],
        in_specs=[in_vmem] * (2 * len(late) + 9) + [anywhere, in_smem],
        out_specs=[anywhere] * 7,
        scratch_shapes=[
            pltpu.VMEM((capacity - ready, row_block, TILE), jnp.float32),
            pltpu.VMEM((3, 4, group, row_block, TILE), jnp.float32),
            pltpu.VMEM((3, *sel_shape), jnp.float32),
            pltpu.SemaphoreType.DMA((1,)),
            pltpu.SemaphoreType.DMA((3, 4)),
            pltpu.SemaphoreType.DMA((4,)),
        ],
        compiler_params=pltpu.CompilerParams(vmem_limit_bytes=update_limit),
    )(
        *lates,
        *kept,
        total,
        sel_sum,
        norm,
        in_hbm(off_states[0]),
        table,
    )
    return (
        news[6],
        *news[:3],
        *(new.reshape(off_weight.shape) for new in news[3:6]),
    )


def solution(mesh):
    placed = (
        P("dp", None),
        P("dp", "tensor"),
        P("tensor", None),
        P("tensor", None, None),
        P("dp", "tensor"),
        P("dp", "tensor"),
        P("dp", "tensor"),
        P("dp", "tensor", None, None, None),
        P("dp", "tensor", None, None, None),
        P("dp", "tensor", None, None, None),
    )
    return jax.shard_map(
        body,
        mesh=mesh,
        in_specs=placed,
        out_specs=(
            P("tensor"),
            P("dp", "tensor"),
            P("dp", "tensor"),
            P("dp", "tensor"),
            P("dp", "tensor", None, None, None),
            P("dp", "tensor", None, None, None),
            P("dp", "tensor", None, None, None),
        ),
        check_vma=False,
    )
```
